32 devices in a mesh: dp: 2 (over x), expert: 16 (over z, y, core).
Axes of the slice: x: 2, y: 2, z: 4, core: 2. Of those that a mesh axis runs over, the one named last changes fastest.
Arguments:
- grad_out: bfloat16 [2048, 7168], P('expert', 'dp'), may hold values from -6 to 6
- expert_ids: int32 [2048, 8], P('expert'), may hold values from 0 to 15, all different within a row; in each aligned block of 128 rows (0 to 127, 128 to 255, ...) at most 80 rows name the same one
- keep: int32 [2048, 8], P('expert'), may hold values 0 or 1
- router_logits: float32 [2048, 8], P('expert'), may hold values from -6 to 6
- w_gate: bfloat16 [16, 7168, 1024], P('expert', 'dp'), may hold values from -0.0625 to 0.0625
- w_up: bfloat16 [16, 7168, 1024], P('expert', 'dp'), may hold values from -0.0625 to 0.0625
- w_down: bfloat16 [16, 1024, 7168], P('expert', None, 'dp'), may hold values from -0.1875 to 0.1875
- saved_gate: bfloat16 [16, 1024, 1280], P('expert', 'dp'), may hold values from -6 to 6
- saved_up: bfloat16 [16, 1024, 1280], P('expert', 'dp'), may hold values from -6 to 6
Outputs:
- grad_tokens: bfloat16 [2048, 7168], P('expert', 'dp')
- router_grad: float32 [2048, 8], P('expert')
The draws below stay inside these ranges and needn't reach their ends.
Inputs may be any that keep to these rules, and one draw needn't show every extreme that they name: `expert_ids`: each token names 8 different experts; the copies that one source's 128 tokens send to one expert number at most 80, and exactly 80 for some source and expert.
All inputs are finite; a program needn't handle non-finite values. No bound on the sum of `keep` on one device may be relied on, other than what follows from the above.
Results may differ from the reference program's by a relative error of at most 0.0065.
Values may be sent and summed in bfloat16 or wider, within the bound.
A program may use at most 128 MiB of HBM per device.

```python
import math
import jax
import jax.numpy as jnp
import numpy as np
from jax import lax

D = 7168
FF = 1024
K = 8
TOK_DEV = 128
EXPERTS = 16
TOKENS = 2048
CAP = 80
SLOTS = 1280
N_EXPERT = 16


def plant(result, rng, low, top_value):
    dims = result.shape
    spot = [jax.random.randint(jax.random.fold_in(rng, axis), (), 0, dims[axis]) for axis in range(len(dims))]
    result = result.at[tuple(spot)].set(low)
    longest = dims.index(max(dims))
    spot[longest] = (spot[longest] + 1) % dims[longest]
    return result.at[tuple(spot)].set(top_value)


def levels(own_key, dims, shards, low, largest):
    loudness = 1.0
    for position, blocks in shards:
        steps = jax.random.uniform(jax.random.fold_in(jax.random.fold_in(own_key, 6), position), (blocks,), jnp.float32, low / len(shards), largest / len(shards))
        loudness = loudness * jnp.repeat(jnp.exp(steps), dims[position] // blocks).reshape((-1,) + (1,) * (len(dims) - 1 - position))
    return loudness


def deal_out(key, own, number, rows, amount, top, most, skew):
    ranking = jax.random.permutation(key, amount)
    packed, usual = shares(amount, rows * top, most, skew, True), shares(amount, rows * top, most, skew, False)
    places = jnp.arange(amount)

    def named(tallies, offset_by):
        used = int((tallies > 0).sum())
        fixed = max(1, used // 4)
        passed = fixed + (places - fixed + offset_by * (used - fixed)) % max(1, amount - fixed)
        return jnp.zeros((amount,), jnp.int32).at[ranking[jnp.where(places < fixed, places, passed)]].set(jnp.asarray(tallies, jnp.int32))

    tallies = jnp.where(number % 4 == 0, named(packed, number // 4), named(usual, number - number // 4 - 1))
    mixed = jax.random.permutation(jax.random.fold_in(own, 3), amount)
    giver, receiver = mixed[0:amount // 2 * 2:2], mixed[1:amount // 2 * 2:2]
    margin = jnp.minimum(tallies[giver] - 1, most - tallies[receiver]) // 2
    margin = jnp.where((giver == ranking[0]) | (receiver == ranking[0]) | (tallies[receiver] == 0), 0, jnp.maximum(margin, 0))
    passed = jax.random.randint(jax.random.fold_in(own, 4), (amount // 2,), 0, 1 << 20) % (margin + 1)
    tallies = tallies.at[giver].add(-passed).at[receiver].add(passed)
    members = jnp.searchsorted(jnp.cumsum(tallies), jnp.arange(rows * top), side="right").astype(jnp.int32)
    listing = members.reshape(top, rows).T
    listing = listing[jax.random.permutation(jax.random.fold_in(own, 1), rows)]
    offset_by = jax.random.randint(jax.random.fold_in(own, 2), (rows, 1), 0, top)
    return jnp.take_along_axis(listing, (jnp.arange(top)[None, :] + offset_by) % top, axis=1)


def shares(amount, total, bound, lean, full):
    loads = [(1 << 20) // math.isqrt(grade ** lean) + 1 for grade in range(1, amount + 1)]
    largest = bound if full else min(bound, max(-(-total // amount), total * loads[0] // sum(loads)))
    least = 1 if total - largest >= amount - 1 else 0
    given, spare = [largest] + [least] * (amount - 1), total - largest - least * (amount - 1)
    while spare > 0:
        free = [i for i in range(1, amount) if given[i] < largest] or [i for i in range(1, amount) if given[i] < bound]
        pool, left = sum([loads[i] for i in free]), spare
        for i in free:
            extra = min(bound - given[i], max(1, left * loads[i] // pool), spare)
            given[i] = given[i] + extra
            spare = spare - extra
    return np.array(given)


def bell_draw(own_key, extent, spread, limit, cuts=(), held_as=jnp.bfloat16):
    level = levels(own_key, extent, cuts, -0.22, 0.18) if cuts else 1.0
    drawn = jax.random.normal(own_key, extent, jnp.float32) * spread * level
    return jnp.minimum(jnp.maximum(drawn, -limit), limit).astype(held_as)


def setup_inputs(seed: int = 0) -> dict:
    seeds = jax.random.split(jax.random.key(seed), 10)
    grad_out = bell_draw(seeds[0], (TOKENS, D), 1.0, 6.0, ((0, 16), (1, 2)))
    expert_ids_keys = jax.random.split(jax.random.fold_in(seeds[1], 1), TOKENS // TOK_DEV)
    expert_ids_turns = jax.random.permutation(jax.random.fold_in(seeds[1], 3), TOKENS // TOK_DEV)
    expert_ids = jax.vmap(lambda own, number: deal_out(jax.random.fold_in(seeds[1], 2), own, number, TOK_DEV, EXPERTS, K, CAP, 2))(expert_ids_keys, expert_ids_turns).reshape((TOKENS, K))
    keep = plant((jax.random.randint(seeds[2], (TOKENS, K), 0, 4) < 3).astype(jnp.int32), jax.random.fold_in(seeds[2], 1), 0, 1)
    router_logits = bell_draw(seeds[3], (TOKENS, K), 1.5, 6.0, ((0, 16),), jnp.float32)
    w_gate = bell_draw(seeds[4], (EXPERTS, D, FF), D ** -0.5, 0.0625, ((0, 16), (1, 2)))
    w_up = bell_draw(seeds[5], (EXPERTS, D, FF), D ** -0.5, 0.0625, ((0, 16), (1, 2)))
    w_down = bell_draw(seeds[6], (EXPERTS, FF, D), FF ** -0.5, 0.1875, ((0, 16), (2, 2)))
    saved_gate = bell_draw(seeds[7], (EXPERTS, FF, SLOTS), 1.5, 6.0, ((0, 16), (1, 2)))
    saved_up = bell_draw(seeds[8], (EXPERTS, FF, SLOTS), 1.0, 6.0, ((0, 16), (1, 2)))
    return dict(grad_out=grad_out, expert_ids=expert_ids, keep=keep, router_logits=router_logits, w_gate=w_gate, w_up=w_up, w_down=w_down, saved_gate=saved_gate, saved_up=saved_up)


routed_scale = 2.5


def positions(ids_block):
    onehot = (ids_block[:, None] == jnp.arange(EXPERTS, dtype=jnp.int32)[None, :]).astype(jnp.int32)
    earlier = jnp.cumsum(onehot, axis=0) - onehot
    return jnp.sum(earlier * onehot, axis=1).astype(jnp.int32)


def reference(grad_out, expert_ids, keep, router_logits, w_gate, w_up, w_down, saved_gate, saved_up):
    ids = expert_ids.reshape(N_EXPERT, TOK_DEV * K).astype(jnp.int32)
    slot = jax.vmap(positions)(ids)
    source = jnp.arange(N_EXPERT, dtype=jnp.int32)[:, None]
    flat = (ids * SLOTS + source * CAP + slot).reshape(-1).astype(jnp.int32)
    token = jnp.repeat(jnp.arange(TOKENS, dtype=jnp.int32), K)
    affinity = jax.nn.sigmoid(router_logits.astype(jnp.float32))
    total = jnp.sum(affinity, axis=1, keepdims=True)
    gate = routed_scale * affinity / total
    keep_f = keep.astype(jnp.float32)
    weight = (gate * keep_f).astype(jnp.bfloat16).astype(jnp.float32)
    table = jnp.full((EXPERTS * SLOTS,), TOKENS, jnp.int32).at[flat].set(token).reshape(EXPERTS, SLOTS)
    weight_table = jnp.zeros((EXPERTS * SLOTS,), jnp.float32).at[flat].set(weight.reshape(-1)).reshape(EXPERTS, SLOTS)
    padded = jnp.concatenate([grad_out, jnp.zeros((1, D), jnp.bfloat16)], axis=0)

    def step(accum, expert):
        index = table[expert]
        rows = padded[index]
        hidden_grad = jnp.dot(rows, w_down[expert].T, preferred_element_type=jnp.float32)
        gate_pre = saved_gate[expert].T.astype(jnp.float32)
        up_pre = saved_up[expert].T.astype(jnp.float32)
        sig = jax.nn.sigmoid(gate_pre)
        act = gate_pre * sig
        act_grad = sig * (1.0 + gate_pre * (1.0 - sig))
        gate_grad = (hidden_grad * up_pre * act_grad).astype(jnp.bfloat16)
        up_grad = (hidden_grad * act).astype(jnp.bfloat16)
        score = jnp.sum(hidden_grad * act * up_pre, axis=1).astype(jnp.bfloat16)
        copy_grad = (jnp.dot(gate_grad, w_gate[expert].T, preferred_element_type=jnp.float32)
                     + jnp.dot(up_grad, w_up[expert].T, preferred_element_type=jnp.float32)).astype(jnp.bfloat16)
        accum = accum.at[index].add(weight_table[expert][:, None] * copy_grad.astype(jnp.float32))
        return accum, score

    accum, scores = lax.scan(step, jnp.zeros((TOKENS + 1, D), jnp.float32), jnp.arange(EXPERTS, dtype=jnp.int32))
    grad_tokens = accum[:TOKENS].astype(jnp.bfloat16)
    copy_score = scores.reshape(-1)[flat].astype(jnp.float32).reshape(TOKENS, K)
    weight_grad = keep_f * copy_score
    mixed = jnp.sum(weight_grad * affinity, axis=1, keepdims=True)
    affinity_grad = routed_scale * (weight_grad / total - mixed / (total * total))
    router_grad = affinity_grad * affinity * (1.0 - affinity)
    return grad_tokens, router_grad
```

```python
import functools
import math

import jax
import jax.numpy as jnp
from jax import lax
from jax.experimental import pallas as pl
from jax.experimental.pallas import tpu as pltpu
from jax.sharding import PartitionSpec as P

routed_scale = 2.5
lanes = 128


def sub_axes(experts):
    cores = 2 if experts % 2 == 0 else 1
    chips = experts // cores
    y = max(1, math.isqrt(max(1, chips // 2)))
    while chips % y:
        y -= 1
    return chips // y, y, cores


class Ring:
    def __init__(self, sizes, which):
        self.sizes, self.which, self.size = sizes, which, sizes[which]

    def move(self, value, step):
        zs, ys, cs = self.sizes
        pairs = []
        for z in range(zs):
            for y in range(ys):
                for c in range(cs):
                    to = [z, y, c]
                    to[self.which] = (to[self.which] + step) % self.size
                    pairs.append(((z * ys + y) * cs + c, (to[0] * ys + to[1]) * cs + to[2]))
        return lax.ppermute(value, "expert", pairs)

    def gather(self, value):
        size, half = self.size, self.size // 2
        blocks = [value] + [None] * (size - 1)
        if size == 2:
            blocks[1] = self.move(value, 1)
            return blocks
        down = up = value
        for d in range(1, half + size % 2):
            down, up = self.move(down, -1), self.move(up, 1)
            blocks[d], blocks[size - d] = down, up
        if size % 2 == 0:
            cut = value.shape[-1] // (2 * lanes) * lanes
            blocks[half] = jnp.concatenate(
                [self.move(down[..., :cut], -1), self.move(up[..., cut:], 1)], axis=-1
            )
        return blocks

    def reduce(self, blocks):
        size, half = self.size, self.size // 2
        total = blocks[0].astype(jnp.float32)
        if size == 1:
            return total
        if size == 2:
            return total + self.move(blocks[1], 1).astype(jnp.float32)
        cut = blocks[0].shape[-1] // (2 * lanes) * lanes
        for direction in (1, -1):
            last = half if size % 2 else half - 1
            held = blocks[direction * last % size]
            if size % 2 == 0:
                far = blocks[half]
                if direction == 1:
                    got = self.move(far[..., :cut], 1).astype(jnp.float32)
                    near = (got + held[..., :cut].astype(jnp.float32)).astype(held.dtype)
                    held = jnp.concatenate([near, held[..., cut:]], axis=-1)
                else:
                    got = self.move(far[..., cut:], -1).astype(jnp.float32)
                    near = (got + held[..., cut:].astype(jnp.float32)).astype(held.dtype)
                    held = jnp.concatenate([held[..., :cut], near], axis=-1)
            for d in range(last - 1, 0, -1):
                got = self.move(held, direction).astype(jnp.float32)
                held = (got + blocks[direction * d % size].astype(jnp.float32)).astype(held.dtype)
            total = total + self.move(held, direction).astype(jnp.float32)
        return total


def shifted(value, axis, size, step):
    return lax.ppermute(value, axis, [(i, (i + step) % size) for i in range(size)])


def whole_over(value, axis):
    size = lax.axis_size(axis)
    index = lax.axis_index(axis)
    part = value.shape[0]
    result = jnp.zeros((part * size,) + value.shape[1:], value.dtype)
    result = lax.dynamic_update_slice(result, value, (index * part, 0))
    for step in range(1, size):
        got = shifted(value, axis, size, step)
        origin = lax.rem(index - step + size, size)
        result = lax.dynamic_update_slice(result, got, (origin * part, 0))
    return result


def contract(grads, columns):
    return lax.dot_general(
        grads, columns, (((0,), (1,)), ((), ())), preferred_element_type=jnp.float32
    )


def by_permutes(
    grad_out, expert_ids, keep, router_logits, w_gate, w_up, w_down, saved_gate, saved_up
):
    experts = lax.axis_size("expert")
    dp = lax.axis_size("dp")
    me = lax.axis_index("expert")
    tok_rows, topk = expert_ids.shape
    slots = saved_gate.shape[2]
    capacity = slots // experts
    width_part = grad_out.shape[1]
    sizes = zs, ys, cs = sub_axes(experts)
    ring_z, ring_y, ring_c = (Ring(sizes, i) for i in range(3))
    cut = -(-width_part * 4 // (7 * lanes)) * lanes

    place = jnp.arange(slots, dtype=jnp.int32)
    block = place // capacity
    dz, dc, dy = block // (cs * ys), block // ys % cs, block % ys
    my_z, my_y, my_c = me // (ys * cs), me // cs % ys, me % cs
    source = ((my_z + dz) % zs * ys + (my_y + dy) % ys) * cs + (my_c + dc) % cs
    slot_of = source * capacity + place % capacity
    reorder = (jnp.arange(slots, dtype=jnp.int32)[:, None] == slot_of[None, :]).astype(jnp.bfloat16)
    gate_pre = whole_over(jnp.dot(saved_gate[0], reorder), "dp")
    up_pre = whole_over(jnp.dot(saved_up[0], reorder), "dp")

    affinity = jax.nn.sigmoid(router_logits)
    total = jnp.sum(affinity, axis=1, keepdims=True)
    gate = routed_scale * affinity / total
    keep_f = keep.astype(jnp.float32)
    weight = (gate * keep_f).astype(jnp.bfloat16)
    extra = -(-2 * topk // lanes) * lanes
    info = jnp.concatenate([expert_ids.astype(jnp.bfloat16), weight], axis=1)
    info = jnp.pad(info, ((0, 0), (0, extra - 2 * topk)))

    first = jnp.stack(ring_y.gather(grad_out[:, :cut]))
    first = ring_z.gather(first)
    first = [ring_c.gather(part) for part in first]
    second = ring_z.gather(jnp.concatenate([grad_out[:, cut:], info], axis=1))
    second = [[list(t) for t in zip(*[ring_c.gather(p) for p in ring_y.gather(part)])] for part in second]

    tail = width_part - cut
    infos = jnp.stack([p[:, tail:] for by_c in second for by_y in by_c for p in by_y])
    hit = infos[..., :topk] == me.astype(jnp.bfloat16)
    mine = jnp.any(hit, axis=2)
    mine_weight = jnp.sum(
        jnp.where(hit, infos[..., topk : 2 * topk].astype(jnp.float32), 0.0), axis=2
    )
    before = jnp.arange(tok_rows)[:, None] < jnp.arange(tok_rows)[None, :]
    position = jnp.dot(
        mine.astype(jnp.bfloat16), before.astype(jnp.bfloat16), preferred_element_type=jnp.float32
    ).astype(jnp.int32)
    route = mine[:, None, :] & (
        position[:, None, :] == jnp.arange(capacity, dtype=jnp.int32)[None, :, None]
    )
    combine = jnp.where(route, mine_weight[:, None, :], 0.0).astype(jnp.bfloat16)
    route = route.astype(jnp.bfloat16)

    def rows_of(pieces):
        return lax.dot_general(
            route, pieces, (((2,), (1,)), ((0,), (0,))), preferred_element_type=jnp.float32
        ).astype(jnp.bfloat16).reshape(slots, -1)

    def down(rows, span):
        return lax.dot_general(
            w_down[0, :, span], rows, (((1,), (1,)), ((), ())), preferred_element_type=jnp.float32
        )

    head_span, tail_span = slice(0, cut), slice(cut, width_part)
    first = jnp.concatenate([p for by_c in first for p in by_c])
    second = jnp.stack([p[:, :tail] for by_c in second for by_y in by_c for p in by_y])
    first, second, gate_pre, up_pre = lax.optimization_barrier((first, second, gate_pre, up_pre))
    partial = down(rows_of(first), head_span) + down(rows_of(second), tail_span)
    sent = partial.astype(jnp.bfloat16)
    hidden = partial
    for shift in range(1, dp):
        hidden = hidden + shifted(sent, "dp", dp, shift).astype(jnp.float32)

    gate_f = gate_pre.astype(jnp.float32)
    up_f = up_pre.astype(jnp.float32)
    sig = jax.nn.sigmoid(gate_f)
    act = gate_f * sig
    act_grad = sig * (1.0 + gate_f * (1.0 - sig))
    gate_grad = (hidden * up_f * act_grad).astype(jnp.bfloat16)
    up_grad = (hidden * act).astype(jnp.bfloat16)
    score = jnp.sum(hidden * act * up_f, axis=0).astype(jnp.bfloat16).reshape(experts, capacity)
    mine_score = jnp.sum(route.astype(jnp.float32) * score.astype(jnp.float32)[:, :, None], axis=1)
    scores = jnp.where(hit, mine_score[:, :, None], 0.0).astype(jnp.bfloat16)
    scores = jnp.pad(scores, ((0, 0), (0, 0), (0, extra - topk)))

    def shares(span, gate_grad, up_grad):
        copy_grad = contract(gate_grad, w_gate[0, span]) + contract(up_grad, w_up[0, span])
        copy_grad = copy_grad.astype(jnp.bfloat16).reshape(experts, capacity, -1)
        return lax.dot_general(
            combine, copy_grad, (((1,), (1,)), ((0,), (0,))), preferred_element_type=jnp.float32
        ).astype(jnp.bfloat16)

    def over_cores(share):
        share = share.reshape(zs, cs, ys, tok_rows, share.shape[-1])
        return ring_c.reduce([share[:, c] for c in range(cs)]).astype(jnp.bfloat16)

    lead = shares(head_span, gate_grad, up_grad)
    lead, gate_grad, up_grad = lax.optimization_barrier((lead, gate_grad, up_grad))
    lead = over_cores(lead)
    last = over_cores(jnp.concatenate([shares(tail_span, gate_grad, up_grad), scores], axis=2))
    lead = ring_z.reduce([lead[z] for z in range(zs)]).astype(jnp.bfloat16)
    lead = ring_y.reduce([lead[y] for y in range(ys)])
    last = ring_y.reduce([last[:, y] for y in range(ys)]).astype(jnp.bfloat16)
    last = ring_z.reduce([last[z] for z in range(zs)])
    grad_tokens = jnp.concatenate([lead, last[:, :tail]], axis=1).astype(jnp.bfloat16)

    weight_grad = keep_f * last[:, tail : tail + topk]
    mixed = jnp.sum(weight_grad * affinity, axis=1, keepdims=True)
    affinity_grad = routed_scale * (weight_grad / total - mixed / (total * total))
    router_grad = affinity_grad * affinity * (1.0 - affinity)
    return (grad_tokens, router_grad)


MESH = pl.DeviceIdType.MESH
unit_lanes = 256
vmem_bytes = 67043328


class Plan:
    def __init__(self, experts, dp, tokens, topk, width, hidden, part, slots):
        self.zs, self.ys, self.cs = sub_axes(experts)
        self.experts, self.tokens, self.topk = experts, tokens, topk
        self.width, self.hidden, self.part, self.slots = width, hidden, part, slots
        self.cap = slots // experts
        self.per_plane = self.ys * self.cs
        self.unit = self.cap * self.per_plane
        units = width // unit_lanes
        lead = max(1, round(units / 6))
        rest = units - lead
        sizes = [lead] + [rest // 3 + (i < rest % 3) for i in range(3)]
        starts = [sum(sizes[:i]) * unit_lanes for i in range(4)]
        self.pieces = [(s, n * unit_lanes) for s, n in zip(starts, sizes)]
        self.lead = lead * unit_lanes
        self.fits = (
            self.ys == 2 and self.cs == 2 and dp == 2 and 2 <= self.zs <= 4
            and width % unit_lanes == 0 and units >= 4 and width <= 3584 and hidden <= 1024
            and self.cap % 16 == 0 and self.cap <= 80 and tokens == lanes and slots % lanes == 0
            and part * dp == hidden and part % unit_lanes == 0
            and topk == 8 and experts % 8 == 0
        )
        self.orders = [
            sorted(range(self.zs), key=lambda other: abs(other - z)) for z in range(self.zs)
        ]

    def place(self):
        me = lax.axis_index("expert")
        return me // (self.ys * self.cs), me // self.cs % self.ys, me % self.cs

    def order(self, z, i):
        result = jnp.int32(self.orders[0][i])
        for at in range(1, self.zs):
            result = jnp.where(z == at, jnp.int32(self.orders[at][i]), result)
        return result

    def at(self, z, y, c):
        return {"expert": (z * self.ys + y) * self.cs + c}

    def span(self, p):
        return pl.ds(self.pieces[p][0], self.pieces[p][1])


def remote(src, dst, send, recv, device):
    return pltpu.make_async_remote_copy(
        src_ref=src, dst_ref=dst, send_sem=send, recv_sem=recv, device_id=device, device_id_type=MESH
    )


def tile_at(q, size):
    return pl.ds(pl.multiple_of(q * size, size), size)


def dispatch_kernel(
    plan, x_hbm, info_ref, wd_hbm, sg_hbm, su_hbm, gu_hbm, comb_ref, score_ref,
    g, info, wd, sg, su, sgt, sut, mine, wrow, pos, rows, ps, pr, hf, gu, scs, sct, scx, sst, scr,
    loc, out_s, info_s, info_r, z_s, y_s, ag_r, d_s, d_r, ps_s, ps_r, gu_s, gu_r, sx_s, sx_r, sc_s, sc_r,
):
    zs, cap, part = plan.zs, plan.cap, plan.part
    tokens, topk, experts, group = plan.tokens, plan.topk, plan.experts, plan.per_plane
    span, parts = plan.span, len(plan.pieces)
    z, y, c = plan.place()
    me = lax.axis_index("expert")
    x = lax.axis_index("dp")
    across = {"dp": 1 - x}

    held = [
        pltpu.make_async_copy(x_hbm, g.at[me], loc.at[0]),
        pltpu.make_async_copy(sg_hbm, sg, loc.at[1]),
        pltpu.make_async_copy(su_hbm, su, loc.at[2]),
        pltpu.make_async_copy(wd_hbm, wd, loc.at[3]),
    ]
    for copy in held:
        copy.start()

    barrier = pltpu.get_barrier_semaphore()

    def greet(i, carry):
        peer = lax.rem(me + i, experts)
        pl.semaphore_signal(barrier, inc=1, device_id={"expert": peer}, device_id_type=MESH)
        return carry

    lax.fori_loop(1, experts, greet, 0)
    pl.semaphore_signal(barrier, inc=1, device_id=across, device_id_type=MESH)
    info[me] = info_ref[...]
    pl.semaphore_wait(barrier, experts)

    def info_copy(peer, slot):
        return remote(info_ref, info.at[slot], info_s.at[peer], info_r.at[slot], {"expert": peer})

    def z_copy(step, b, p):
        ref = g.at[b * 2 + c, :, span(p)]
        way = 0 if step < 0 else 1
        return remote(ref, ref, z_s.at[way, b, p], ag_r.at[b, p], plan.at(z + step, y, c))

    def y_copy(b, p):
        ref = g.at[b * 2 + c, :, span(p)]
        return remote(ref, ref, y_s.at[b, p], ag_r.at[b, p], plan.at(z, 1 - y, c))

    def d_copy(b, p, core):
        ref = g.at[b * 2 + core, :, span(p)]
        return remote(ref, ref, d_s.at[b, p], d_r.at[b, p], plan.at(z, y, 1 - c))

    def ps_copy(i):
        return remote(ps.at[i], pr.at[i], ps_s.at[i], ps_r.at[i], across)

    def gu_copy(i, k, half):
        at = pl.ds(pl.multiple_of(k * plan.hidden + half * part, lanes), part)
        ref = gu.at[i, :, at]
        return remote(ref, ref, gu_s.at[i, k], gu_r.at[i, k], across)

    def sx_copy(i):
        return remote(sct.at[i], scx.at[i], sx_s.at[i], sx_r.at[i], across)

    def sc_copy(i, target, slot):
        return remote(sst.at[i], scr.at[slot], sc_s.at[target], sc_r.at[slot], {"expert": target})

    def out_copy(i):
        return pltpu.make_async_copy(gu.at[i], gu_hbm.at[i], out_s.at[i])

    def send_info(i, carry):
        info_copy(lax.rem(me + i, experts), me).start()
        return carry

    lax.fori_loop(1, experts, send_info, 0)

    def toward(side, b, p):
        @pl.when((z + side >= 0) & (z + side < zs))
        def _():
            z_copy(side, b, p).start()

    held[0].wait()
    own, beside = z * 2 + y, z * 2 + 1 - y
    y_copy(own, 0).start()
    for p in list(range(1, parts)) + [0]:
        for side in (-1, 1):
            toward(side, own, p)
        if p:
            y_copy(own, p).start()
    for p in range(parts):
        d_copy(own, p, c).start()

    held[1].wait()
    held[2].wait()

    def turn(k, carry):
        at = tile_at(k, lanes)
        sgt[at, :] = sg[:, at].T
        sut[at, :] = su[:, at].T
        return carry

    lax.fori_loop(0, plan.slots // lanes, turn, 0)

    def wait_info(i, carry):
        slot = lax.rem(me + i, experts)
        info_copy(slot, slot).wait_recv()
        return carry

    lax.fori_loop(1, experts, wait_info, 0)
    for s in range(experts):
        both = info[s].astype(jnp.float32)
        hit = both[:topk] == me.astype(jnp.float32)
        mine[s : s + 1, :] = jnp.max(jnp.where(hit, 1.0, 0.0), axis=0, keepdims=True)
        wrow[s : s + 1, :] = jnp.sum(
            jnp.where(hit, both[topk : 2 * topk], 0.0), axis=0, keepdims=True
        )
    before = lax.broadcasted_iota(jnp.int32, (tokens, tokens), 0) < lax.broadcasted_iota(
        jnp.int32, (tokens, tokens), 1
    )
    chosen = mine[...]
    count = jnp.dot(
        chosen.astype(jnp.bfloat16),
        jnp.where(before, 1.0, 0.0).astype(jnp.bfloat16),
        preferred_element_type=jnp.float32,
    )
    pos[...] = jnp.where(chosen > 0.0, count, -1.0)

    def z_events(d, chosen_parts):
        rows_of = [(p, y) for p in chosen_parts if p]
        if 0 in chosen_parts:
            rows_of += [(0, y), (0, 1 - y)]
        for p, row in rows_of:
            for side in (-1, 1):
                from_z = z + side * d

                @pl.when((from_z >= 0) & (from_z < zs))
                def _(p=p, row=row, side=side, from_z=from_z):
                    b = from_z * 2 + row
                    y_copy(b, p).wait_recv()
                    toward(-side, b, p)
                    if p:
                        y_copy(b, p).start()
                    d_copy(b, p, c).start()

    def y_events(d):
        for p in range(1, parts):
            for side in (-1, 1) if d else (1,):
                from_z = z + side * d

                @pl.when((from_z >= 0) & (from_z < zs))
                def _(p=p, from_z=from_z):
                    b = from_z * 2 + 1 - y
                    y_copy(b, p).wait_recv()
                    d_copy(b, p, c).start()

    def route_of(s):
        slot = lax.broadcasted_iota(jnp.int32, (cap, tokens), 0).astype(jnp.float32)
        return slot == pos[pl.ds(s, 1), :]

    def process(i):
        plane = plan.order(z, i)
        for row in range(2):
            for p in range(parts):
                d_copy(plane * 2 + row, p, 1 - c).wait_recv()

        def gather(j, carry):
            s = plane * group + j
            route = route_of(s)
            comb_ref[i, j] = jnp.where(route, wrow[pl.ds(s, 1), :], 0.0).astype(jnp.bfloat16)
            route = jnp.where(route, 1.0, 0.0).astype(jnp.bfloat16)
            at_rows = pl.ds(pl.multiple_of(j * cap, 16), cap)

            def step(q, carry):
                at = tile_at(q, unit_lanes)
                rows[at_rows, at] = jnp.dot(
                    route, g[s, :, at], preferred_element_type=jnp.float32
                ).astype(jnp.bfloat16)
                return carry

            return lax.fori_loop(0, plan.width // unit_lanes, step, carry)

        lax.fori_loop(0, group, gather, 0)
        if i == 0:
            held[3].wait()

        def down(half, keep):
            def step(n, carry):
                at = tile_at(n, unit_lanes)
                first = pl.multiple_of(half * part + n * unit_lanes, unit_lanes)
                value = lax.dot_general(
                    rows[...], wd[pl.ds(first, unit_lanes), :], (((1,), (1,)), ((), ())),
                    preferred_element_type=jnp.float32,
                )
                if keep:
                    hf[i, :, at] = value
                else:
                    ps[i, :, at] = value.astype(jnp.bfloat16)
                return carry

            lax.fori_loop(0, part // unit_lanes, step, 0)

        down(1 - x, False)
        ps_copy(i).start()
        down(x, True)

    chunk = 16

    def act(i):
        plane = plan.order(z, i)
        ps_copy(i).wait_recv()

        def step(k, carry):
            at = tile_at(k, chunk)
            src = pl.ds(pl.multiple_of(plane * plan.unit + k * chunk, chunk), chunk)
            hid = hf[i, at, :] + pr[i, at, :].astype(jnp.float32)
            gate = sgt[src, :].astype(jnp.float32)
            up = sut[src, :].astype(jnp.float32)
            sig = 1.0 / (1.0 + jnp.exp(-gate))
            value = gate * sig
            slope = sig * (1.0 + gate * (1.0 - sig))
            grad = hid * value
            lower = pl.multiple_of(x * part, lanes)
            upper = pl.multiple_of(plan.hidden + x * part, lanes)
            gu[i, at, pl.ds(lower, part)] = (hid * up * slope).astype(jnp.bfloat16)
            gu[i, at, pl.ds(upper, part)] = grad.astype(jnp.bfloat16)
            scs[at, :] = jnp.broadcast_to(jnp.sum(grad * up, axis=1, keepdims=True), (chunk, lanes))
            return carry

        lax.fori_loop(0, plan.unit // chunk, step, 0)
        for k in range(2):
            gu_copy(i, k, x).start()
        sct[i] = jnp.zeros((8, tokens), jnp.float32)
        for j in range(group):
            route = route_of(plane * group + j)
            value = jnp.where(route, scs[j * cap : (j + 1) * cap, :], 0.0)
            sct[i, j : j + 1, :] = jnp.sum(value, axis=0, keepdims=True)
        sx_copy(i).start()

    def finish(i):
        plane = plan.order(z, i)
        for k in range(2):
            gu_copy(i, k, 1 - x).wait_recv()
        out_copy(i).start()
        sx_copy(i).wait_recv()
        sst[i] = sct[i] + scx[i]
        if i == 0:
            scr[me] = sct[i] + scx[i]
        for j in range(group):
            target = plane * group + j
            if i == 0:
                @pl.when(target != me)
                def _(target=target):
                    sc_copy(i, target, me).start()
            else:
                sc_copy(i, target, me).start()

    every = list(range(parts))
    y_copy(beside, 0).wait_recv()
    for side in (-1, 1):
        toward(side, beside, 0)
    d_copy(beside, 0, c).start()
    z_events(1, every)
    y_events(0)
    process(0)
    if zs > 2:
        z_events(2, every)
    y_events(1)
    process(1)
    act(0)
    if zs == 3:
        y_events(2)
        process(2)
        act(1)
    if zs == 4:
        z_events(3, [1, 2])
        at_end = (z == 0) | (z == zs - 1)
        pl.when(at_end)(lambda: y_events(2))
        process(2)
        z_events(3, [3, 0])
        act(1)
        pl.when(jnp.logical_not(at_end))(lambda: y_events(2))
        finish(0)
        y_events(3)
        process(3)
        act(2)
    act(zs - 1)
    for i in range(1 if zs == 4 else 0, zs):
        finish(i)

    def wait_scores(i, carry):
        peer = lax.rem(me + i, experts)
        sc_copy(0, peer, peer).wait_recv()
        sc_copy(0, peer, me).wait_send()
        info_copy(peer, me).wait_send()
        return carry

    lax.fori_loop(1, experts, wait_scores, 0)
    row = me % group
    for s in range(experts):
        score_ref[s : s + 1, :] = scr[s, pl.ds(row, 1), :]
    for b_z in range(zs):
        for b_y in range(2):
            b = b_z * 2 + b_y
            for p in range(parts):
                d_copy(b, p, c).wait_send()
                crosses = (y == b_y) if p else ((y == b_y) & (z == b_z))

                @pl.when(crosses)
                def _(b=b, p=p):
                    y_copy(b, p).wait_send()

                for side in (-1, 1):
                    goes = (z >= b_z) if side > 0 else (z <= b_z)
                    goes = goes & (z + side >= 0) & (z + side < zs)
                    if p:
                        goes = goes & (y == b_y)

                    @pl.when(goes)
                    def _(b=b, p=p, side=side):
                        z_copy(side, b, p).wait_send()

    for i in range(zs):
        ps_copy(i).wait_send()
        sx_copy(i).wait_send()
        for k in range(2):
            gu_copy(i, k, x).wait_send()
        out_copy(i).wait()


def return_kernel(
    plan, gu_hbm, comb, wg_hbm, wu_hbm, out_ref,
    wg, wu, gu, cg, t, sd, dr, yr, zra, zrb,
    w_l, gu_l, d_s, d_r, y_s, y_r, za_s, za_r, zb_s, zb_r,
):
    zs, cap, hidden = plan.zs, plan.cap, plan.hidden
    span, pieces, parts = plan.span, plan.pieces, len(plan.pieces)
    z, y, c = plan.place()
    f32, bf16 = jnp.float32, jnp.bfloat16

    gu_in = [pltpu.make_async_copy(gu_hbm.at[i], gu.at[i], gu_l.at[i]) for i in range(zs)]
    w_in = [
        [pltpu.make_async_copy(hbm.at[span(p), :], ref.at[span(p), :], w_l.at[k, p])
         for k, (hbm, ref) in enumerate([(wg_hbm, wg), (wu_hbm, wu)])]
        for p in range(parts)
    ]
    gu_in[zs - 1].start()
    for pair in w_in:
        for copy in pair:
            copy.start()
    for i in reversed(range(zs - 1)):
        gu_in[i].start()

    barrier = pltpu.get_barrier_semaphore()

    def signal(device):
        pl.semaphore_signal(barrier, inc=1, device_id=device, device_id_type=MESH)

    signal(plan.at(z, 1 - y, c))
    signal(plan.at(z, y, 1 - c))
    pl.when(z > 0)(lambda: signal(plan.at(z - 1, y, c)))
    pl.when(z < zs - 1)(lambda: signal(plan.at(z + 1, y, c)))
    pl.semaphore_wait(barrier, 2 + jnp.minimum(z, 1) + jnp.minimum(zs - 1 - z, 1))

    def d_copy(i, row, p):
        return remote(
            sd.at[i, row, :, span(p)], dr.at[i, row, :, span(p)],
            d_s.at[i, row, p], d_r.at[i, row, p], plan.at(z, y, 1 - c),
        )

    def y_copy(i, p):
        return remote(
            t.at[i, 1 - y, :, span(p)], yr.at[i, :, span(p)],
            y_s.at[i, p], y_r.at[i, p], plan.at(z, 1 - y, c),
        )

    def late(p):
        return pl.ds(pieces[p][0] - plan.lead, pieces[p][1])

    def z_copy(i, row, p, slot, device):
        if p:
            return remote(
                t.at[i, y, :, span(p)], zrb.at[slot, :, late(p)],
                zb_s.at[i, p], zb_r.at[slot, p], device,
            )
        return remote(
            t.at[i, row, :, span(0)], zra.at[slot, row], za_s.at[i, row], za_r.at[slot, row], device
        )

    def tiles(p, body):
        first, size = pieces[p]

        def step(q, carry):
            at = pl.ds(pl.multiple_of(first + q * unit_lanes, unit_lanes), unit_lanes)
            near = pl.ds(
                pl.multiple_of(first - (plan.lead if p else 0) + q * unit_lanes, unit_lanes), unit_lanes
            )
            body(at, near)
            return carry

        lax.fori_loop(0, size // unit_lanes, step, 0)

    def grads(i, p):
        if i == zs - 1:
            for copy in w_in[p]:
                copy.wait()
        if p == 0:
            gu_in[i].wait()

        def body(at, near):
            value = lax.dot_general(
                gu[i, :, :hidden], wg[at, :], (((1,), (1,)), ((), ())), preferred_element_type=f32
            ) + lax.dot_general(
                gu[i, :, hidden:], wu[at, :], (((1,), (1,)), ((), ())), preferred_element_type=f32
            )
            cg[...] = value.astype(bf16)
            for ref, core in ((sd, 1 - c), (t, c)):
                for row in range(2):
                    j = row * 2 + core
                    ref[i, row, :, at] = lax.dot_general(
                        comb[i, j], cg[pl.ds(pl.multiple_of(j * cap, 16), cap), :],
                        (((0,), (0,)), ((), ())), preferred_element_type=f32,
                    ).astype(bf16)

        tiles(p, body)
        for row in range(2):
            d_copy(i, row, p).start()

    def over_cores(i, p):
        for row in range(2):
            d_copy(i, row, p).wait_recv()

        def body(at, near):
            for row in range(2):
                t[i, row, :, at] = (
                    t[i, row, :, at].astype(f32) + dr[i, row, :, at].astype(f32)
                ).astype(bf16)

        tiles(p, body)
        if p:
            y_copy(i, p).start()

    def hop(i):
        plane = plan.order(z, i)
        above = plane > z
        step = jnp.where(above, 1, -1)
        fed = (above & (z > 0)) | (jnp.logical_not(above) & (z < zs - 1))
        last = z + step == plane
        slot = jnp.where(last & jnp.logical_not(above), zs, plane)
        return plane, fed, slot, plan.at(z + step, y, c)

    def along(i, p):
        plane, fed, slot, device = hop(i)
        which = [y] if p else [0, 1]
        if p:
            y_copy(i, p).wait_recv()

        def add(with_z):
            if with_z:
                for row in which:
                    z_copy(i, row, p, plane, device).wait_recv()

            def body(at, near):
                for row in which:
                    value = t[i, row, :, at].astype(f32)
                    if p:
                        value = value + yr[i, :, at].astype(f32)
                    if with_z:
                        got = zrb[plane, :, near] if p else zra[plane, row, :, near]
                        value = value + got.astype(f32)
                    t[i, row, :, at] = value.astype(bf16)

            tiles(p, body)

        pl.when(fed)(lambda: add(True))
        if p:
            pl.when(jnp.logical_not(fed))(lambda: add(False))
        for row in which:
            z_copy(i, row, p, slot, device).start()

    def arrivals(p):
        device = plan.at(z, y, 1 - c)
        for slot, there in ((z, z > 0), (zs, z < zs - 1)):
            for row in ([y] if p else [0, 1]):
                @pl.when(there)
                def _(slot=slot, row=row):
                    z_copy(0, row, p, slot, device).wait_recv()

    def from_planes(p, row, near):
        total = None
        for slot, there in ((z, z > 0), (zs, z < zs - 1)):
            got = zrb[slot, :, near] if p else zra[slot, row, :, near]
            got = jnp.where(there, got.astype(f32), 0.0)
            total = got if total is None else total + got
        return total

    def own_lead():
        arrivals(0)

        def body(at, near):
            t[0, 1 - y, :, at] = (
                t[0, 1 - y, :, at].astype(f32) + from_planes(0, 1 - y, near)
            ).astype(bf16)

        tiles(0, body)
        y_copy(0, 0).start()

    def own(p):
        if p:
            arrivals(p)
        y_copy(0, p).wait_recv()

        def body(at, near):
            value = t[0, y, :, at].astype(f32) + yr[0, :, at].astype(f32)
            out_ref[:, at] = (value + from_planes(p, y, near)).astype(bf16)

        tiles(p, body)

    steps = [(i, p) for i in reversed(range(zs)) for p in range(parts)]
    lag = 3
    for k in range(len(steps) + lag):
        if k < len(steps):
            grads(*steps[k])
        if 0 <= k - 1 < len(steps):
            over_cores(*steps[k - 1])
        if 0 <= k - lag < len(steps) and steps[k - lag][0]:
            along(*steps[k - lag])
    own_lead()
    for p in list(range(1, parts)) + [0]:
        own(p)

    for i in range(zs):
        for p in range(parts):
            for row in range(2):
                d_copy(i, row, p).wait_send()
            if p or not i:
                y_copy(i, p).wait_send()
            if i:
                plane, fed, slot, device = hop(i)
                for row in [y] if p else [0, 1]:
                    z_copy(i, row, p, slot, device).wait_send()


def by_kernels(
    plan, grad_out, expert_ids, keep, router_logits, w_gate, w_up, w_down, saved_gate, saved_up
):
    zs, experts, tokens, topk = plan.zs, plan.experts, plan.tokens, plan.topk
    width, hidden, part, unit, group = plan.width, plan.hidden, plan.part, plan.unit, plan.per_plane
    parts = len(plan.pieces)
    bf16, f32 = jnp.bfloat16, jnp.float32
    any_, in_vmem = pl.BlockSpec(memory_space=pl.ANY), pl.BlockSpec(memory_space=pltpu.VMEM)
    dma = pltpu.SemaphoreType.DMA

    affinity = jax.nn.sigmoid(router_logits)
    total = jnp.sum(affinity, axis=1, keepdims=True)
    keep_f = keep.astype(f32)
    weight = (routed_scale * affinity / total * keep_f).astype(bf16)
    info = jnp.concatenate([expert_ids.astype(bf16), weight], axis=1).T

    sent = 128 * width * 2
    gu, comb, score = pl.pallas_call(
        functools.partial(dispatch_kernel, plan),
        name="dispatch_kernel",
        out_shape=(
            jax.ShapeDtypeStruct((zs, unit, 2 * hidden), bf16),
            jax.ShapeDtypeStruct((zs, group, plan.cap, tokens), bf16),
            jax.ShapeDtypeStruct((experts, tokens), f32),
        ),
        in_specs=[any_, in_vmem, any_, any_, any_],
        out_specs=(any_, in_vmem, in_vmem),
        scratch_shapes=[
            pltpu.VMEM((experts, tokens, width), bf16),
            pltpu.VMEM((experts, 2 * topk, tokens), bf16),
            pltpu.VMEM((hidden, width), bf16),
            pltpu.VMEM((part, plan.slots), bf16),
            pltpu.VMEM((part, plan.slots), bf16),
            pltpu.VMEM((plan.slots, part), bf16),
            pltpu.VMEM((plan.slots, part), bf16),
            pltpu.VMEM((experts, tokens), f32),
            pltpu.VMEM((experts, tokens), f32),
            pltpu.VMEM((experts, tokens), f32),
            pltpu.VMEM((unit, width), bf16),
            pltpu.VMEM((zs, unit, part), bf16),
            pltpu.VMEM((zs, unit, part), bf16),
            pltpu.VMEM((zs, unit, part), f32),
            pltpu.VMEM((zs, unit, 2 * hidden), bf16),
            pltpu.VMEM((unit, lanes), f32),
            pltpu.VMEM((zs, 8, tokens), f32),
            pltpu.VMEM((zs, 8, tokens), f32),
            pltpu.VMEM((zs, 8, tokens), f32),
            pltpu.VMEM((experts, 8, tokens), f32),
            dma((4,)), dma((zs,)), dma((experts,)), dma((experts,)),
            dma((2, 2 * zs, parts)), dma((2 * zs, parts)), dma((2 * zs, parts)),
            dma((2 * zs, parts)), dma((2 * zs, parts)),
            dma((zs,)), dma((zs,)), dma((zs, 2)), dma((zs, 2)), dma((zs,)), dma((zs,)),
            dma((experts,)), dma((experts,)),
        ],
        compiler_params=pltpu.CompilerParams(
            collective_id=0, has_side_effects=True, vmem_limit_bytes=vmem_bytes
        ),
        cost_estimate=pl.CostEstimate(
            flops=2 * plan.slots * width * (hidden + tokens), transcendentals=0,
            bytes_accessed=2 * (hidden * width + experts * tokens * width),
        ),
    )(grad_out, info, w_down[0], saved_gate[0], saved_up[0])

    grad_tokens = pl.pallas_call(
        functools.partial(return_kernel, plan),
        name="return_kernel",
        out_shape=jax.ShapeDtypeStruct((tokens, width), bf16),
        in_specs=[any_, in_vmem, any_, any_],
        out_specs=in_vmem,
        scratch_shapes=[
            pltpu.VMEM((width, hidden), bf16),
            pltpu.VMEM((width, hidden), bf16),
            pltpu.VMEM((zs, unit, 2 * hidden), bf16),
            pltpu.VMEM((unit, unit_lanes), bf16),
            pltpu.VMEM((zs, 2, tokens, width), bf16),
            pltpu.VMEM((zs, 2, tokens, width), bf16),
            pltpu.VMEM((zs, 2, tokens, width), bf16),
            pltpu.VMEM((zs, tokens, width), bf16),
            pltpu.VMEM((zs + 1, 2, tokens, plan.lead), bf16),
            pltpu.VMEM((zs + 1, tokens, width - plan.lead), bf16),
            dma((2, parts)), dma((zs,)),
            dma((zs, 2, parts)), dma((zs, 2, parts)), dma((zs, parts)), dma((zs, parts)),
            dma((zs, 2)), dma((zs + 1, 2)), dma((zs, parts)), dma((zs + 1, parts)),
        ],
        compiler_params=pltpu.CompilerParams(
            collective_id=1, has_side_effects=True, vmem_limit_bytes=vmem_bytes
        ),
        cost_estimate=pl.CostEstimate(
            flops=2 * plan.slots * width * (2 * hidden + tokens), transcendentals=0,
            bytes_accessed=4 * hidden * width,
        ),
    )(gu, comb, w_gate[0], w_up[0])

    chosen = expert_ids[:, :, None] == jnp.arange(experts, dtype=jnp.int32)
    mine = jnp.sum(jnp.where(chosen, score.T[:, None, :], 0.0), axis=2)
    weight_grad = keep_f * lax.reduce_precision(mine, 8, 7)
    mixed = jnp.sum(weight_grad * affinity, axis=1, keepdims=True)
    affinity_grad = routed_scale * (weight_grad / total - mixed / (total * total))
    return (grad_tokens, affinity_grad * affinity * (1.0 - affinity))


def on_device(grad_out, expert_ids, keep, router_logits, w_gate, w_up, w_down, saved_gate, saved_up):
    plan = Plan(
        lax.axis_size("expert"), lax.axis_size("dp"), *expert_ids.shape, grad_out.shape[1],
        w_down.shape[1], saved_gate.shape[1], saved_gate.shape[2],
    )
    form = functools.partial(by_kernels, plan) if plan.fits else by_permutes
    return form(
        grad_out, expert_ids, keep, router_logits, w_gate, w_up, w_down, saved_gate, saved_up
    )


def solution(mesh):
    in_specs = (
        P("expert", "dp"),
        P("expert", None),
        P("expert", None),
        P("expert", None),
        P("expert", "dp", None),
        P("expert", "dp", None),
        P("expert", None, "dp"),
        P("expert", "dp", None),
        P("expert", "dp", None),
    )
    out_specs = (P("expert", "dp"), P("expert", None))
    return jax.shard_map(
        on_device, mesh=mesh, in_specs=in_specs, out_specs=out_specs, check_vma=False
    )
```

```python
import functools
import math

import jax
import jax.numpy as jnp
from jax import lax
from jax.experimental import pallas as pl
from jax.experimental.pallas import tpu as pltpu
from jax.sharding import PartitionSpec as P

routed_scale = 2.5
lanes = 128


def sub_axes(experts):
    cores = 2 if experts % 2 == 0 else 1
    chips = experts // cores
    y = max(1, math.isqrt(max(1, chips // 2)))
    while chips % y:
        y -= 1
    return chips // y, y, cores


class Ring:
    def __init__(self, sizes, which):
        self.sizes, self.which, self.size = sizes, which, sizes[which]

    def move(self, value, step):
        zs, ys, cs = self.sizes
        pairs = []
        for z in range(zs):
            for y in range(ys):
                for c in range(cs):
                    to = [z, y, c]
                    to[self.which] = (to[self.which] + step) % self.size
                    pairs.append(((z * ys + y) * cs + c, (to[0] * ys + to[1]) * cs + to[2]))
        return lax.ppermute(value, "expert", pairs)

    def gather(self, value):
        size, half = self.size, self.size // 2
        blocks = [value] + [None] * (size - 1)
        if size == 2:
            blocks[1] = self.move(value, 1)
            return blocks
        down = up = value
        for d in range(1, half + size % 2):
            down, up = self.move(down, -1), self.move(up, 1)
            blocks[d], blocks[size - d] = down, up
        if size % 2 == 0:
            cut = value.shape[-1] // (2 * lanes) * lanes
            blocks[half] = jnp.concatenate(
                [self.move(down[..., :cut], -1), self.move(up[..., cut:], 1)], axis=-1
            )
        return blocks

    def reduce(self, blocks):
        size, half = self.size, self.size // 2
        total = blocks[0].astype(jnp.float32)
        if size == 1:
            return total
        if size == 2:
            return total + self.move(blocks[1], 1).astype(jnp.float32)
        cut = blocks[0].shape[-1] // (2 * lanes) * lanes
        for direction in (1, -1):
            last = half if size % 2 else half - 1
            held = blocks[direction * last % size]
            if size % 2 == 0:
                far = blocks[half]
                if direction == 1:
                    got = self.move(far[..., :cut], 1).astype(jnp.float32)
                    near = (got + held[..., :cut].astype(jnp.float32)).astype(held.dtype)
                    held = jnp.concatenate([near, held[..., cut:]], axis=-1)
                else:
                    got = self.move(far[..., cut:], -1).astype(jnp.float32)
                    near = (got + held[..., cut:].astype(jnp.float32)).astype(held.dtype)
                    held = jnp.concatenate([held[..., :cut], near], axis=-1)
            for d in range(last - 1, 0, -1):
                got = self.move(held, direction).astype(jnp.float32)
                held = (got + blocks[direction * d % size].astype(jnp.float32)).astype(held.dtype)
            total = total + self.move(held, direction).astype(jnp.float32)
        return total


def shifted(value, axis, size, step):
    return lax.ppermute(value, axis, [(i, (i + step) % size) for i in range(size)])


def whole_over(value, axis):
    size = lax.axis_size(axis)
    index = lax.axis_index(axis)
    part = value.shape[0]
    result = jnp.zeros((part * size,) + value.shape[1:], value.dtype)
    result = lax.dynamic_update_slice(result, value, (index * part, 0))
    for step in range(1, size):
        got = shifted(value, axis, size, step)
        origin = lax.rem(index - step + size, size)
        result = lax.dynamic_update_slice(result, got, (origin * part, 0))
    return result


def contract(grads, columns):
    return lax.dot_general(
        grads, columns, (((0,), (1,)), ((), ())), preferred_element_type=jnp.float32
    )


def by_permutes(
    grad_out, expert_ids, keep, router_logits, w_gate, w_up, w_down, saved_gate, saved_up
):
    experts = lax.axis_size("expert")
    dp = lax.axis_size("dp")
    me = lax.axis_index("expert")
    tok_rows, topk = expert_ids.shape
    slots = saved_gate.shape[2]
    capacity = slots // experts
    width_part = grad_out.shape[1]
    sizes = zs, ys, cs = sub_axes(experts)
    ring_z, ring_y, ring_c = (Ring(sizes, i) for i in range(3))
    cut = -(-width_part * 4 // (7 * lanes)) * lanes

    place = jnp.arange(slots, dtype=jnp.int32)
    block = place // capacity
    dz, dc, dy = block // (cs * ys), block // ys % cs, block % ys
    my_z, my_y, my_c = me // (ys * cs), me // cs % ys, me % cs
    source = ((my_z + dz) % zs * ys + (my_y + dy) % ys) * cs + (my_c + dc) % cs
    slot_of = source * capacity + place % capacity
    reorder = (jnp.arange(slots, dtype=jnp.int32)[:, None] == slot_of[None, :]).astype(jnp.bfloat16)
    gate_pre = whole_over(jnp.dot(saved_gate[0], reorder), "dp")
    up_pre = whole_over(jnp.dot(saved_up[0], reorder), "dp")

    affinity = jax.nn.sigmoid(router_logits)
    total = jnp.sum(affinity, axis=1, keepdims=True)
    gate = routed_scale * affinity / total
    keep_f = keep.astype(jnp.float32)
    weight = (gate * keep_f).astype(jnp.bfloat16)
    extra = -(-2 * topk // lanes) * lanes
    info = jnp.concatenate([expert_ids.astype(jnp.bfloat16), weight], axis=1)
    info = jnp.pad(info, ((0, 0), (0, extra - 2 * topk)))

    first = jnp.stack(ring_y.gather(grad_out[:, :cut]))
    first = ring_z.gather(first)
    first = [ring_c.gather(part) for part in first]
    second = ring_z.gather(jnp.concatenate([grad_out[:, cut:], info], axis=1))
    second = [[list(t) for t in zip(*[ring_c.gather(p) for p in ring_y.gather(part)])] for part in second]

    tail = width_part - cut
    infos = jnp.stack([p[:, tail:] for by_c in second for by_y in by_c for p in by_y])
    hit = infos[..., :topk] == me.astype(jnp.bfloat16)
    mine = jnp.any(hit, axis=2)
    mine_weight = jnp.sum(
        jnp.where(hit, infos[..., topk : 2 * topk].astype(jnp.float32), 0.0), axis=2
    )
    before = jnp.arange(tok_rows)[:, None] < jnp.arange(tok_rows)[None, :]
    position = jnp.dot(
        mine.astype(jnp.bfloat16), before.astype(jnp.bfloat16), preferred_element_type=jnp.float32
    ).astype(jnp.int32)
    route = mine[:, None, :] & (
        position[:, None, :] == jnp.arange(capacity, dtype=jnp.int32)[None, :, None]
    )
    combine = jnp.where(route, mine_weight[:, None, :], 0.0).astype(jnp.bfloat16)
    route = route.astype(jnp.bfloat16)

    def rows_of(pieces):
        return lax.dot_general(
            route, pieces, (((2,), (1,)), ((0,), (0,))), preferred_element_type=jnp.float32
        ).astype(jnp.bfloat16).reshape(slots, -1)

    def down(rows, span):
        return lax.dot_general(
            w_down[0, :, span], rows, (((1,), (1,)), ((), ())), preferred_element_type=jnp.float32
        )

    head_span, tail_span = slice(0, cut), slice(cut, width_part)
    first = jnp.concatenate([p for by_c in first for p in by_c])
    second = jnp.stack([p[:, :tail] for by_c in second for by_y in by_c for p in by_y])
    first, second, gate_pre, up_pre = lax.optimization_barrier((first, second, gate_pre, up_pre))
    partial = down(rows_of(first), head_span) + down(rows_of(second), tail_span)
    sent = partial.astype(jnp.bfloat16)
    hidden = partial
    for shift in range(1, dp):
        hidden = hidden + shifted(sent, "dp", dp, shift).astype(jnp.float32)

    gate_f = gate_pre.astype(jnp.float32)
    up_f = up_pre.astype(jnp.float32)
    sig = jax.nn.sigmoid(gate_f)
    act = gate_f * sig
    act_grad = sig * (1.0 + gate_f * (1.0 - sig))
    gate_grad = (hidden * up_f * act_grad).astype(jnp.bfloat16)
    up_grad = (hidden * act).astype(jnp.bfloat16)
    score = jnp.sum(hidden * act * up_f, axis=0).astype(jnp.bfloat16).reshape(experts, capacity)
    mine_score = jnp.sum(route.astype(jnp.float32) * score.astype(jnp.float32)[:, :, None], axis=1)
    scores = jnp.where(hit, mine_score[:, :, None], 0.0).astype(jnp.bfloat16)
    scores = jnp.pad(scores, ((0, 0), (0, 0), (0, extra - topk)))

    def shares(span, gate_grad, up_grad):
        copy_grad = contract(gate_grad, w_gate[0, span]) + contract(up_grad, w_up[0, span])
        copy_grad = copy_grad.astype(jnp.bfloat16).reshape(experts, capacity, -1)
        return lax.dot_general(
            combine, copy_grad, (((1,), (1,)), ((0,), (0,))), preferred_element_type=jnp.float32
        ).astype(jnp.bfloat16)

    def over_cores(share):
        share = share.reshape(zs, cs, ys, tok_rows, share.shape[-1])
        return ring_c.reduce([share[:, c] for c in range(cs)]).astype(jnp.bfloat16)

    lead = shares(head_span, gate_grad, up_grad)
    lead, gate_grad, up_grad = lax.optimization_barrier((lead, gate_grad, up_grad))
    lead = over_cores(lead)
    last = over_cores(jnp.concatenate([shares(tail_span, gate_grad, up_grad), scores], axis=2))
    lead = ring_z.reduce([lead[z] for z in range(zs)]).astype(jnp.bfloat16)
    lead = ring_y.reduce([lead[y] for y in range(ys)])
    last = ring_y.reduce([last[:, y] for y in range(ys)]).astype(jnp.bfloat16)
    last = ring_z.reduce([last[z] for z in range(zs)])
    grad_tokens = jnp.concatenate([lead, last[:, :tail]], axis=1).astype(jnp.bfloat16)

    weight_grad = keep_f * last[:, tail : tail + topk]
    mixed = jnp.sum(weight_grad * affinity, axis=1, keepdims=True)
    affinity_grad = routed_scale * (weight_grad / total - mixed / (total * total))
    router_grad = affinity_grad * affinity * (1.0 - affinity)
    return (grad_tokens, router_grad)


MESH = pl.DeviceIdType.MESH
unit_lanes = 256
vmem_bytes = 67043328


class Plan:
    def __init__(self, experts, dp, tokens, topk, width, hidden, part, slots):
        self.zs, self.ys, self.cs = sub_axes(experts)
        self.experts, self.tokens, self.topk = experts, tokens, topk
        self.width, self.hidden, self.part, self.slots = width, hidden, part, slots
        self.cap = slots // experts
        self.per_plane = self.ys * self.cs
        self.unit = self.cap * self.per_plane
        units = width // unit_lanes
        lead = max(1, round(units / 5))
        rest = units - lead
        sizes = [lead] + [rest // 3 + (i < rest % 3) for i in range(3)]
        starts = [sum(sizes[:i]) * unit_lanes for i in range(4)]
        self.pieces = [(s, n * unit_lanes) for s, n in zip(starts, sizes)]
        self.lead = lead * unit_lanes
        self.wide = unit_lanes * (2 if units % 2 == 0 else 1)
        self.widest = max(sizes) * unit_lanes
        self.fits = (
            self.ys == 2 and self.cs == 2 and dp == 2 and self.zs == 4
            and width % unit_lanes == 0 and units >= 4 and width <= 3584 and hidden <= 1024
            and self.cap % 16 == 0 and self.cap <= 80 and tokens == lanes and slots % lanes == 0
            and part * dp == hidden and part % unit_lanes == 0
            and topk == 8 and experts % 8 == 0
        )
        self.orders = [
            sorted(range(self.zs), key=lambda other: (abs(other - z), abs(2 * other - self.zs + 1)))
            for z in range(self.zs)
        ]

    def place(self):
        me = lax.axis_index("expert")
        return me // (self.ys * self.cs), me // self.cs % self.ys, me % self.cs

    def order(self, z, i):
        result = jnp.int32(self.orders[0][i])
        for at in range(1, self.zs):
            result = jnp.where(z == at, jnp.int32(self.orders[at][i]), result)
        return result

    def at(self, z, y, c):
        return {"expert": (z * self.ys + y) * self.cs + c}

    def span(self, p):
        return pl.ds(self.pieces[p][0], self.pieces[p][1])


def remote(src, dst, send, recv, device):
    return pltpu.make_async_remote_copy(
        src_ref=src, dst_ref=dst, send_sem=send, recv_sem=recv, device_id=device, device_id_type=MESH
    )


def tile_at(q, size):
    return pl.ds(pl.multiple_of(q * size, size), size)


def layer_kernel(
    plan, x_hbm, info_ref, wd_hbm, sg_hbm, su_hbm, wg_hbm, wu_hbm, out_ref, score_ref,
    g, info, wd, sg, su, sgt, sut, sgo, suo, mine, wrow, pos, rows, ps, pr, hf, gu, comb,
    scs, sct, scx, sst, scr, wt, cg, sd, yr, zra, zrb,
    loc, info_s, info_r, z_s, y_s, ag_r, d_s, d_r, so_s, so_r, ps_s, ps_r, gu_s, gu_r,
    sx_s, sx_r, sc_s, sc_r, w_l, free, h_s, h_r, ry_s, ry_r, za_s, za_r, zb_s, zb_r,
):
    zs, cap, part, hidden, unit = plan.zs, plan.cap, plan.part, plan.hidden, plan.unit
    tokens, topk, experts, group = plan.tokens, plan.topk, plan.experts, plan.per_plane
    span, pieces, parts = plan.span, plan.pieces, len(plan.pieces)
    f32, bf16 = jnp.float32, jnp.bfloat16
    z, y, c = plan.place()
    me = lax.axis_index("expert")
    x = lax.axis_index("dp")
    across = {"dp": 1 - x}
    at_end = (z == 0) | (z == zs - 1)
    inside = jnp.logical_not(at_end)

    held = [
        pltpu.make_async_copy(x_hbm, g.at[me], loc.at[0]),
        pltpu.make_async_copy(sg_hbm, sg, loc.at[1]),
        pltpu.make_async_copy(su_hbm, su, loc.at[2]),
        pltpu.make_async_copy(wd_hbm, wd, loc.at[3]),
    ]
    for copy in held:
        copy.start()

    barrier = pltpu.get_barrier_semaphore()

    def greet(i, carry):
        peer = lax.rem(me + i, experts)
        pl.semaphore_signal(barrier, inc=1, device_id={"expert": peer}, device_id_type=MESH)
        return carry

    lax.fori_loop(1, experts, greet, 0)
    pl.semaphore_signal(barrier, inc=1, device_id=across, device_id_type=MESH)
    info[me] = info_ref[...]
    pl.semaphore_wait(barrier, experts)

    def info_copy(peer, slot):
        return remote(info_ref, info.at[slot], info_s.at[peer], info_r.at[slot], {"expert": peer})

    def z_copy(step, b, p):
        ref = g.at[b * 2 + c, :, span(p)]
        way = 0 if step < 0 else 1
        return remote(ref, ref, z_s.at[way, b, p], ag_r.at[b, p], plan.at(z + step, y, c))

    def y_copy(b, p):
        ref = g.at[b * 2 + c, :, span(p)]
        return remote(ref, ref, y_s.at[b, p], ag_r.at[b, p], plan.at(z, 1 - y, c))

    def d_copy(b, p, core):
        ref = g.at[b * 2 + core, :, span(p)]
        return remote(ref, ref, d_s.at[b, p], d_r.at[b, p], plan.at(z, y, 1 - c))

    def so_copy(i, k):
        src = (sgt, sut)[k].at[pl.ds(pl.multiple_of(plan.order(z, i) * unit, 16), unit), :]
        return remote(src, (sgo, suo)[k].at[i - 1], so_s.at[i - 1, k], so_r.at[i - 1, k], across)

    def half_at(half, offset=0):
        return pl.ds(pl.multiple_of(offset + half * part, lanes), part)

    def ps_copy(i, half, which):
        at = half_at(half)
        return remote(ps.at[i, :, at], pr.at[i, :, at], ps_s.at[i, which], ps_r.at[i, which], across)

    def gu_copy(k, half):
        ref = gu.at[0, :, half_at(half, k * hidden)]
        return remote(ref, ref, gu_s.at[k], gu_r.at[k], across)

    def sx_copy(i):
        return remote(sct.at[i], scx.at[i], sx_s.at[i], sx_r.at[i], across)

    def sc_copy(i, target, slot):
        return remote(sst.at[i], scr.at[slot], sc_s.at[target], sc_r.at[slot], {"expert": target})

    def send_info(i, carry):
        info_copy(lax.rem(me + i, experts), me).start()
        return carry

    lax.fori_loop(1, experts, send_info, 0)

    def toward(side, b, p):
        @pl.when((z + side >= 0) & (z + side < zs))
        def _():
            z_copy(side, b, p).start()

    held[0].wait()
    own_b, beside = z * 2 + y, z * 2 + 1 - y
    y_copy(own_b, 0).start()
    for p in list(range(1, parts)) + [0]:
        for side in (-1, 1):
            toward(side, own_b, p)
        if p:
            y_copy(own_b, p).start()
    for p in range(parts):
        d_copy(own_b, p, c).start()

    tiles_all = plan.width // unit_lanes
    ring = wt.shape[0]
    total_tiles = tiles_all * zs

    def w_copy(n, k):
        tile = lax.rem(n, tiles_all)
        slot = lax.rem(n, ring)
        return pltpu.make_async_copy(
            (wg_hbm, wu_hbm)[k].at[tile_at(tile, unit_lanes), :], wt.at[slot, :, pl.ds(k * hidden, hidden)],
            w_l.at[slot, k],
        )

    for n in range(ring - 1):
        for k in range(2):
            w_copy(jnp.int32(n), k).start()

    held[1].wait()
    held[2].wait()

    def turn(k, carry):
        at = tile_at(k, lanes)
        sgt[at, :] = sg[:, at].T
        sut[at, :] = su[:, at].T
        return carry

    lax.fori_loop(0, plan.slots // lanes, turn, 0)
    for i in range(1, zs - 1):
        for k in range(2):
            so_copy(i, k).start()

    def wait_info(i, carry):
        slot = lax.rem(me + i, experts)
        info_copy(slot, slot).wait_recv()
        return carry

    lax.fori_loop(1, experts, wait_info, 0)
    for s in range(experts):
        both = info[s].astype(f32)
        hit = both[:topk] == me.astype(f32)
        mine[s : s + 1, :] = jnp.max(jnp.where(hit, 1.0, 0.0), axis=0, keepdims=True)
        wrow[s : s + 1, :] = jnp.sum(
            jnp.where(hit, both[topk : 2 * topk], 0.0), axis=0, keepdims=True
        )
    before = lax.broadcasted_iota(jnp.int32, (tokens, tokens), 0) < lax.broadcasted_iota(
        jnp.int32, (tokens, tokens), 1
    )
    chosen = mine[...]
    count = jnp.dot(
        chosen.astype(bf16), jnp.where(before, 1.0, 0.0).astype(bf16), preferred_element_type=f32
    )
    pos[...] = jnp.where(chosen > 0.0, count, -1.0)

    def z_events(d, chosen_parts):
        rows_of = [(p, y) for p in chosen_parts if p]
        if 0 in chosen_parts:
            rows_of += [(0, y), (0, 1 - y)]
        for p, row in rows_of:
            for side in (-1, 1):
                from_z = z + side * d

                @pl.when((from_z >= 0) & (from_z < zs))
                def _(p=p, row=row, side=side, from_z=from_z):
                    b = from_z * 2 + row
                    y_copy(b, p).wait_recv()
                    toward(-side, b, p)
                    if p:
                        y_copy(b, p).start()
                    d_copy(b, p, c).start()

    def y_events(d):
        for p in range(1, parts):
            for side in (-1, 1) if d else (1,):
                from_z = z + side * d

                @pl.when((from_z >= 0) & (from_z < zs))
                def _(p=p, from_z=from_z):
                    b = from_z * 2 + 1 - y
                    y_copy(b, p).wait_recv()
                    d_copy(b, p, c).start()

    def route_of(s):
        slot = lax.broadcasted_iota(jnp.int32, (cap, tokens), 0).astype(f32)
        return slot == pos[pl.ds(s, 1), :]

    def process(i):
        plane = plan.order(z, i)
        for row in range(2):
            for p in range(parts):
                d_copy(plane * 2 + row, p, 1 - c).wait_recv()

        routes = []
        for j in range(group):
            s = plane * group + j
            route = route_of(s)
            comb[i, j] = jnp.where(route, wrow[pl.ds(s, 1), :], 0.0).T.astype(bf16)
            routes.append(jnp.where(route, 1.0, 0.0).astype(bf16))

        def gather(q, carry):
            at = tile_at(q, plan.wide)
            for j in range(group):
                rows[j * cap : (j + 1) * cap, at] = jnp.dot(
                    routes[j], g[plane * group + j, :, at], preferred_element_type=f32
                ).astype(bf16)
            return carry

        lax.fori_loop(0, plan.width // plan.wide, gather, 0)
        pl.semaphore_signal(
            free.at[i], inc=1, device_id=plan.at(z, y, 1 - c), device_id_type=MESH
        )
        if i == 0:
            held[3].wait()
        for which, half in enumerate((1 - x, x)):
            def step(n, carry, which=which, half=half):
                first = pl.multiple_of(half * part + n * unit_lanes, unit_lanes)
                value = lax.dot_general(
                    rows[...], wd[pl.ds(first, unit_lanes), :], (((1,), (1,)), ((), ())),
                    preferred_element_type=f32,
                )
                at = pl.ds(first, unit_lanes)
                if i or which:
                    hf[i, :, at] = value
                if i or not which:
                    ps[i, :, at] = value.astype(bf16)
                return carry

            lax.fori_loop(0, part // unit_lanes, step, 0)
            if i or not which:
                ps_copy(i, half, which).start()

    chunk = 32 if unit % 32 == 0 else 16

    def act(i):
        plane = plan.order(z, i)
        ps_copy(i, x, 0).wait_recv()
        for which, half in enumerate((x, 1 - x) if i else (x,)):
            if which:
                ps_copy(i, half, 1).wait_recv()
                for k in range(2):
                    so_copy(i, k).wait_recv()

            def step(k, carry, which=which, half=half):
                at = tile_at(k, chunk)
                lower, upper = half_at(half), half_at(half, hidden)
                hid = hf[i, at, lower] + pr[i, at, lower].astype(f32)
                if which:
                    gate, up = sgo[i - 1, at, :].astype(f32), suo[i - 1, at, :].astype(f32)
                else:
                    src = pl.ds(pl.multiple_of(plane * unit + k * chunk, chunk), chunk)
                    gate, up = sgt[src, :].astype(f32), sut[src, :].astype(f32)
                sig = 1.0 / (1.0 + jnp.exp(-gate))
                value = gate * sig
                slope = sig * (1.0 + gate * (1.0 - sig))
                grad = hid * value
                gu[i, at, lower] = (hid * up * slope).astype(bf16)
                gu[i, at, upper] = grad.astype(bf16)
                if not which:
                    scs[at, :] = jnp.broadcast_to(
                        jnp.sum(grad * up, axis=1, keepdims=True), (chunk, lanes)
                    )
                return carry

            lax.fori_loop(0, unit // chunk, step, 0)
        if i == 0:
            for k in range(2):
                gu_copy(k, x).start()
        sct[i] = jnp.zeros((8, tokens), f32)
        for j in range(group):
            value = jnp.where(route_of(plane * group + j), scs[j * cap : (j + 1) * cap, :], 0.0)
            sct[i, j : j + 1, :] = jnp.sum(value, axis=0, keepdims=True)
        sx_copy(i).start()

    def send_scores(i):
        plane = plan.order(z, i)
        sx_copy(i).wait_recv()
        sst[i] = sct[i] + scx[i]
        if i == 0:
            scr[me] = sct[i] + scx[i]
        for j in range(group):
            target = plane * group + j
            if i == 0:
                pl.when(target != me)(functools.partial(lambda to: sc_copy(i, to, me).start(), target))
            else:
                sc_copy(i, target, me).start()

    def mine_at(i, row, at):
        return g.at[(plan.order(z, i) * 2 + row) * 2 + c, :, at]

    def settle(i):
        plane = plan.order(z, i)
        for row in range(2):
            b = plane * 2 + row
            for p in range(parts):
                came = i == 0
                crosses = (y == row) if p else ((y == row) & came)
                d_copy(b, p, c).wait_send()
                if p or came:
                    pl.when(y == row)(functools.partial(lambda b, p: y_copy(b, p).wait_send(), b, p))
                for side in (-1, 1):
                    goes = (z >= plane) if side > 0 else (z <= plane)
                    goes = goes & (z + side >= 0) & (z + side < zs)
                    if p:
                        goes = goes & (y == row)
                    pl.when(goes)(functools.partial(
                        lambda side, b, p: z_copy(side, b, p).wait_send(), side, b, p
                    ))

    def h_copy(i, row, p):
        size = pieces[p][1]
        plane = plan.order(z, i)
        return remote(
            sd.at[p % 2, row, :, pl.ds(0, size)],
            g.at[(plane * 2 + row) * 2 + c, :, span(p)],
            h_s.at[p % 2, row], h_r.at[i, row, p], plan.at(z, y, 1 - c),
        )

    def ry_copy(i, p):
        return remote(
            mine_at(i, 1 - y, span(p)), yr.at[i, :, span(p)], ry_s.at[i, p], ry_r.at[i, p],
            plan.at(z, 1 - y, c),
        )

    def late(p):
        return pl.ds(pieces[p][0] - plan.lead, pieces[p][1])

    def rz_copy(i, row, p, slot, device):
        if p:
            return remote(
                mine_at(i, y, span(p)), zrb.at[slot, :, late(p)],
                zb_s.at[i, p], zb_r.at[slot, p], device,
            )
        return remote(
            mine_at(i, row, span(0)), zra.at[slot, row], za_s.at[i, row], za_r.at[slot, row], device
        )

    def tiles(p, body):
        first, size = pieces[p]

        def step(q, carry):
            near = tile_at(q, unit_lanes)
            at = pl.ds(pl.multiple_of(first + q * unit_lanes, unit_lanes), unit_lanes)
            far = pl.ds(
                pl.multiple_of(first - (plan.lead if p else 0) + q * unit_lanes, unit_lanes), unit_lanes
            )
            body(first // unit_lanes + q, at, near, far)
            return carry

        lax.fori_loop(0, size // unit_lanes, step, 0)

    runs = []
    busy = [None, None]

    def grads(i, p):
        if p == 0:
            settle(i)
            pl.semaphore_wait(free.at[i], 1)
            runs.append(i)
        base = (len(runs) - 1) * tiles_all
        plane = plan.order(z, i)
        if busy[p % 2] is not None:
            for row in range(2):
                h_copy(busy[p % 2][0], row, busy[p % 2][1]).wait_send()
        busy[p % 2] = (i, p)

        first = pieces[p][0] // unit_lanes

        def multiply(q):
            n = base + first + q

            @pl.when(n + ring - 1 < total_tiles)
            def _():
                for k in range(2):
                    w_copy(n + ring - 1, k).start()

            for k in range(2):
                w_copy(n, k).wait()
            return lax.dot_general(
                gu[i], wt[lax.rem(n, ring)], (((1,), (1,)), ((), ())), preferred_element_type=f32
            )

        def scatter(q):
            at, near = tile_at(first + q, unit_lanes), tile_at(q, unit_lanes)
            for core in (1 - c, c):
                for row in range(2):
                    j = row * 2 + core
                    share = jnp.dot(
                        comb[i, j], cg[pl.ds(pl.multiple_of(j * cap, 16), cap), :],
                        preferred_element_type=f32,
                    ).astype(bf16)
                    if core is c:
                        g[(plane * 2 + row) * 2 + c, :, at] = share
                    else:
                        sd[p % 2, row, :, near] = share

        def step(q, carry):
            value = multiply(q)
            scatter(q - 1)
            cg[...] = value.astype(bf16)
            return carry

        cg[...] = multiply(0).astype(bf16)
        count_p = pieces[p][1] // unit_lanes
        lax.fori_loop(1, count_p, step, 0)
        scatter(count_p - 1)
        for row in range(2):
            h_copy(i, row, p).start()

    def over_cores(i, p):
        for row in range(2):
            h_copy(i, row, p).wait_recv()
        plane = plan.order(z, i)

        def body(q, at, near, far):
            for row in range(2):
                s = (plane * 2 + row) * 2
                g[s + c, :, at] = (
                    g[s + c, :, at].astype(f32) + g[s + 1 - c, :, at].astype(f32)
                ).astype(bf16)

        tiles(p, body)
        if p:
            ry_copy(i, p).start()

    def hop(i):
        plane = plan.order(z, i)
        above = plane > z
        step = jnp.where(above, 1, -1)
        last = z + step == plane
        slot = jnp.where(last & jnp.logical_not(above), zs, plane)
        return plane, slot, plan.at(z + step, y, c)

    def along(i, p, fed):
        plane, slot, device = hop(i)
        which = [y] if p else [0, 1]
        if p:
            ry_copy(i, p).wait_recv()
        if fed:
            for row in which:
                rz_copy(i, row, p, plane, device).wait_recv()

        def body(q, at, near, far):
            for row in which:
                s = (plane * 2 + row) * 2 + c
                value = g[s, :, at].astype(f32)
                if p:
                    value = value + yr[i, :, at].astype(f32)
                if fed:
                    got = zrb[plane, :, far] if p else zra[plane, row, :, far]
                    value = value + got.astype(f32)
                g[s, :, at] = value.astype(bf16)

        if p or fed:
            tiles(p, body)
        for row in which:
            rz_copy(i, row, p, slot, device).start()

    def arrivals(p):
        device = plan.at(z, y, 1 - c)
        for slot, there in ((z, z > 0), (zs, z < zs - 1)):
            for row in ([y] if p else [0, 1]):
                pl.when(there)(functools.partial(
                    lambda slot, row: rz_copy(0, row, p, slot, device).wait_recv(), slot, row
                ))

    def from_planes(p, row, far):
        total = None
        for slot, there in ((z, z > 0), (zs, z < zs - 1)):
            got = zrb[slot, :, far] if p else zra[slot, row, :, far]
            got = jnp.where(there, got.astype(f32), 0.0)
            total = got if total is None else total + got
        return total

    def own_lead():
        arrivals(0)
        s = beside * 2 + c

        def body(q, at, near, far):
            g[s, :, at] = (g[s, :, at].astype(f32) + from_planes(0, 1 - y, far)).astype(bf16)

        tiles(0, body)
        ry_copy(0, 0).start()

    def own(p):
        if p:
            arrivals(p)
        ry_copy(0, p).wait_recv()

        def body(q, at, near, far):
            value = g[me, :, at].astype(f32) + yr[0, :, at].astype(f32)
            out_ref[:, at] = (value + from_planes(p, y, far)).astype(bf16)

        tiles(p, body)

    def back(i, between=None, after=None):
        for k in range(parts + 2):
            if k < parts:
                grads(i, k)
                if between:
                    between(k)
            if 0 <= k - 1 < parts:
                over_cores(i, k - 1)
            if i and 0 <= k - 2 < parts:
                pl.when(at_end)(functools.partial(along, i, k - 2, False))
                if after:
                    after(k - 2)

    every = list(range(parts))
    y_copy(beside, 0).wait_recv()
    for side in (-1, 1):
        toward(side, beside, 0)
    d_copy(beside, 0, c).start()
    z_events(1, every)
    y_events(0)
    process(0)
    pl.when(at_end)(lambda: y_events(1))

    @pl.when(inside)
    def _():
        z_events(2, every)
        y_events(1)

    process(1)
    for k in range(2):
        so_copy(zs - 1, k).start()

    @pl.when(at_end)
    def _():
        z_events(2, every)
        y_events(2)

    process(2)
    z_events(3, [1])
    act(1)
    back(1, between=lambda k: z_events(3, {0: [2], 1: [3], 2: [0], 3: []}[k]))
    pl.when(inside)(lambda: y_events(2))
    y_events(3)
    process(3)
    act(0)
    act(2)
    back(2)
    act(3)
    back(3, after=lambda p: pl.when(inside)(functools.partial(along, 1, p, True)))
    for k in range(2):
        gu_copy(k, 1 - x).wait_recv()
    back(0)
    for i in range(zs):
        send_scores(i)
    for p in range(parts):
        @pl.when(inside)
        def _(p=p):
            along(3, p, True)
            along(2, p, True)
    own_lead()
    for p in list(range(1, parts)) + [0]:
        own(p)

    def wait_scores(i, carry):
        peer = lax.rem(me + i, experts)
        sc_copy(0, peer, peer).wait_recv()
        sc_copy(0, peer, me).wait_send()
        info_copy(peer, me).wait_send()
        return carry

    lax.fori_loop(1, experts, wait_scores, 0)
    row = lax.rem(me, group)
    for s in range(experts):
        score_ref[s : s + 1, :] = scr[s, pl.ds(row, 1), :]
    for i in range(zs):
        sx_copy(i).wait_send()
        for which, half in enumerate((1 - x, x) if i else (1 - x,)):
            ps_copy(i, half, which).wait_send()
        for k in range(2):
            if i:
                so_copy(i, k).wait_send()
            else:
                gu_copy(k, x).wait_send()
        for p in range(parts):
            if p or not i:
                ry_copy(i, p).wait_send()
            if i:
                plane, slot, device = hop(i)
                for row in [y] if p else [0, 1]:
                    rz_copy(i, row, p, slot, device).wait_send()
    for i, p in busy:
        for row in range(2):
            h_copy(i, row, p).wait_send()


def by_kernel(
    plan, grad_out, expert_ids, keep, router_logits, w_gate, w_up, w_down, saved_gate, saved_up
):
    zs, experts, tokens, topk = plan.zs, plan.experts, plan.tokens, plan.topk
    width, hidden, part, unit, group = plan.width, plan.hidden, plan.part, plan.unit, plan.per_plane
    parts = len(plan.pieces)
    bf16, f32 = jnp.bfloat16, jnp.float32
    any_, in_vmem = pl.BlockSpec(memory_space=pl.ANY), pl.BlockSpec(memory_space=pltpu.VMEM)
    dma, vmem = pltpu.SemaphoreType.DMA, pltpu.VMEM

    affinity = jax.nn.sigmoid(router_logits)
    total = jnp.sum(affinity, axis=1, keepdims=True)
    keep_f = keep.astype(f32)
    weight = (routed_scale * affinity / total * keep_f).astype(bf16)
    info = jnp.concatenate([expert_ids.astype(bf16), weight], axis=1).T

    grad_tokens, score = pl.pallas_call(
        functools.partial(layer_kernel, plan),
        name="layer_kernel",
        out_shape=(
            jax.ShapeDtypeStruct((tokens, width), bf16),
            jax.ShapeDtypeStruct((experts, tokens), f32),
        ),
        in_specs=[any_, in_vmem, any_, any_, any_, any_, any_],
        out_specs=(in_vmem, in_vmem),
        scratch_shapes=[
            vmem((experts, tokens, width), bf16),
            vmem((experts, 2 * topk, tokens), bf16),
            vmem((hidden, width), bf16),
            vmem((part, plan.slots), bf16),
            vmem((part, plan.slots), bf16),
            vmem((plan.slots, part), bf16),
            vmem((plan.slots, part), bf16),
            vmem((zs - 1, unit, part), bf16),
            vmem((zs - 1, unit, part), bf16),
            vmem((experts, tokens), f32),
            vmem((experts, tokens), f32),
            vmem((experts, tokens), f32),
            vmem((unit, width), bf16),
            vmem((zs, unit, hidden), bf16),
            vmem((zs, unit, hidden), bf16),
            vmem((zs, unit, hidden), f32),
            vmem((zs, unit, 2 * hidden), bf16),
            vmem((zs, group, tokens, plan.cap), bf16),
            vmem((unit, lanes), f32),
            vmem((zs, 8, tokens), f32),
            vmem((zs, 8, tokens), f32),
            vmem((zs, 8, tokens), f32),
            vmem((experts, 8, tokens), f32),
            vmem((4, unit_lanes, 2 * hidden), bf16),
            vmem((unit, unit_lanes), bf16),
            vmem((2, 2, tokens, plan.widest), bf16),
            vmem((zs, tokens, width), bf16),
            vmem((zs + 1, 2, tokens, plan.lead), bf16),
            vmem((zs + 1, tokens, width - plan.lead), bf16),
            dma((4,)), dma((experts,)), dma((experts,)),
            dma((2, 2 * zs, parts)), dma((2 * zs, parts)), dma((2 * zs, parts)),
            dma((2 * zs, parts)), dma((2 * zs, parts)),
            dma((zs - 1, 2)), dma((zs - 1, 2)), dma((zs, 2)), dma((zs, 2)), dma((2,)), dma((2,)),
            dma((zs,)), dma((zs,)), dma((experts,)), dma((experts,)),
            dma((4, 2)), pltpu.SemaphoreType.REGULAR((zs,)),
            dma((2, 2)), dma((zs, 2, parts)), dma((zs, parts)), dma((zs, parts)),
            dma((zs, 2)), dma((zs + 1, 2)), dma((zs, parts)), dma((zs + 1, parts)),
        ],
        compiler_params=pltpu.CompilerParams(
            collective_id=0, has_side_effects=True, vmem_limit_bytes=vmem_bytes
        ),
        cost_estimate=pl.CostEstimate(
            flops=2 * plan.slots * width * (3 * hidden + 2 * tokens), transcendentals=0,
            bytes_accessed=(2 + 4 * zs) * hidden * width,
        ),
    )(grad_out, info, w_down[0], saved_gate[0], saved_up[0], w_gate[0], w_up[0])

    chosen = expert_ids[:, :, None] == jnp.arange(experts, dtype=jnp.int32)
    mine = jnp.sum(jnp.where(chosen, score.T[:, None, :], 0.0), axis=2)
    weight_grad = keep_f * lax.reduce_precision(mine, 8, 7)
    mixed = jnp.sum(weight_grad * affinity, axis=1, keepdims=True)
    affinity_grad = routed_scale * (weight_grad / total - mixed / (total * total))
    return (grad_tokens, affinity_grad * affinity * (1.0 - affinity))


def on_device(grad_out, expert_ids, keep, router_logits, w_gate, w_up, w_down, saved_gate, saved_up):
    plan = Plan(
        lax.axis_size("expert"), lax.axis_size("dp"), *expert_ids.shape, grad_out.shape[1],
        w_down.shape[1], saved_gate.shape[1], saved_gate.shape[2],
    )
    form = functools.partial(by_kernel, plan) if plan.fits else by_permutes
    return form(
        grad_out, expert_ids, keep, router_logits, w_gate, w_up, w_down, saved_gate, saved_up
    )


def solution(mesh):
    in_specs = (
        P("expert", "dp"),
        P("expert", None),
        P("expert", None),
        P("expert", None),
        P("expert", "dp", None),
        P("expert", "dp", None),
        P("expert", None, "dp"),
        P("expert", "dp", None),
        P("expert", "dp", None),
    )
    out_specs = (P("expert", "dp"), P("expert", None))
    return jax.shard_map(
        on_device, mesh=mesh, in_specs=in_specs, out_specs=out_specs, check_vma=False
    )
```
